32 devices in a mesh: dp: 2 (over x), ep: 4 (over z), tp: 4 (over y, core).
Axes of the slice: x: 2, y: 2, z: 4, core: 2. Of those that a mesh axis runs over, the one named last changes fastest.
Arguments:
- x_in: bfloat16 [32768, 2048], P(('dp', 'ep')), parts along dimension 0
- expert_ids: int32 [32768, 2], P(('dp', 'ep')), parts along dimension 0
- gate_vals: float32 [32768, 2], P(('dp', 'ep')), parts along dimension 0
- w_gate: bfloat16 [8, 2048, 5632], P('ep', None, 'tp')
- w_up: bfloat16 [8, 2048, 5632], P('ep', None, 'tp')
- w_down: bfloat16 [8, 5632, 2048], P('ep', 'tp')
Outputs:
- output: bfloat16 [32768, 2048], P(('dp', 'ep')), parts along dimension 0
There are 2 independent parts. The reference program is written for one: setup_inputs(seed, part) draws one part's arguments, and reference() takes and returns one part's arrays. A program takes and returns all parts, laid end to end along the dimension named above; an argument that names none is the same for every part.
All inputs are finite; a program needn't handle non-finite values.
Results may differ from the reference program's by a relative error of at most 0.00950133.
Values are sent between devices in bfloat16 or wider.
A program may use at most 1 GiB of HBM per device.

```python
import jax
import jax.numpy as jnp
from jax import lax

D = 2048
FF = 5632
EXPERTS = 8
TOP = 2
TOKENS = 4096
SOURCES = 4

CAPACITY = (5 * TOP * TOKENS) // (4 * EXPERTS)


def draw_routing(key, num_rows):
    scores = jax.random.randint(key, (num_rows, EXPERTS), 0, 1048576, dtype=jnp.int32)
    scores = scores * EXPERTS + jnp.arange(EXPERTS, dtype=jnp.int32)[None, :]
    _, chosen = lax.top_k(scores, TOP)
    return chosen.astype(jnp.int32)


def setup_inputs(seed: int = 0, part: int = 0) -> dict:
    base = jax.random.key(seed)
    key_x, key_ids, key_gate = jax.random.split(jax.random.fold_in(base, part), 3)
    key_wg, key_wu, key_wd = jax.random.split(jax.random.key(seed + 1), 3)
    num_rows = SOURCES * TOKENS
    x_in = jax.random.normal(key_x, (num_rows, D), jnp.float32).astype(jnp.bfloat16)
    expert_ids = draw_routing(key_ids, num_rows)
    gate_vals = jax.random.uniform(key_gate, (num_rows, TOP), jnp.float32, 0.25, 1.25)
    w_gate = (jax.random.normal(key_wg, (EXPERTS, D, FF), jnp.float32) * D ** -0.5).astype(jnp.bfloat16)
    w_up = (jax.random.normal(key_wu, (EXPERTS, D, FF), jnp.float32) * D ** -0.5).astype(jnp.bfloat16)
    w_down = (jax.random.normal(key_wd, (EXPERTS, FF, D), jnp.float32) * FF ** -0.5).astype(jnp.bfloat16)
    return {'x_in': x_in, 'expert_ids': expert_ids, 'gate_vals': gate_vals,
            'w_gate': w_gate, 'w_up': w_up, 'w_down': w_down}


def slot_numbers(ids_one):
    flat_ids = ids_one.reshape(TOKENS * TOP)
    onehot = (flat_ids[:, None] == jnp.arange(EXPERTS, dtype=jnp.int32)[None, :]).astype(jnp.int32)
    slots = jnp.sum((jnp.cumsum(onehot, axis=0) - onehot) * onehot, axis=1)
    return slots.reshape(TOKENS, TOP)


def reference(x_in, expert_ids, gate_vals, w_gate, w_up, w_down):
    x_src = x_in.reshape(SOURCES, TOKENS, D)
    ids_src = expert_ids.reshape(SOURCES, TOKENS, TOP)
    gates_src = gate_vals.reshape(SOURCES, TOKENS, TOP)
    slots = lax.map(slot_numbers, ids_src)
    kept = slots < CAPACITY
    flat_slot = jnp.where(kept, ids_src * CAPACITY + slots, EXPERTS * CAPACITY)
    token_num = jnp.broadcast_to(jnp.arange(TOKENS, dtype=jnp.int32)[:, None], (TOKENS, TOP))

    def dispatch(operands):
        tok_rows, slot_one = operands
        slot_owner = jnp.full((EXPERTS * CAPACITY + 1,), TOKENS, jnp.int32)
        slot_owner = slot_owner.at[slot_one.reshape(TOKENS * TOP)].set(token_num.reshape(TOKENS * TOP))
        padded = jnp.concatenate([tok_rows, jnp.zeros((1, D), tok_rows.dtype)], axis=0)
        return padded[slot_owner[: EXPERTS * CAPACITY]]

    slot_rows = lax.map(dispatch, (x_src, flat_slot))
    by_expert = slot_rows.reshape(SOURCES, EXPERTS, CAPACITY, D).transpose(1, 0, 2, 3)
    by_expert = by_expert.reshape(EXPERTS, SOURCES * CAPACITY, D)

    def expert_ffn(operands):
        rows_e, wg_e, wu_e, wd_e = operands
        gated = jax.nn.silu(jnp.dot(rows_e, wg_e, preferred_element_type=jnp.float32)) * jnp.dot(rows_e, wu_e, preferred_element_type=jnp.float32)
        hidden = gated.astype(jnp.bfloat16)
        return jnp.dot(hidden, wd_e, preferred_element_type=jnp.float32).astype(jnp.bfloat16)

    y_rows = lax.map(expert_ffn, (by_expert, w_gate, w_up, w_down))
    y_src = y_rows.reshape(EXPERTS, SOURCES, CAPACITY, D).transpose(1, 0, 2, 3)
    y_src = y_src.reshape(SOURCES, EXPERTS * CAPACITY, D)

    def combine(operands):
        y_one, slot_one, gate_one, kept_one = operands
        safe_slot = jnp.minimum(slot_one, EXPERTS * CAPACITY - 1)
        weight = jnp.where(kept_one, gate_one, 0.0)
        total = jnp.zeros((TOKENS, D), jnp.float32)
        for choice in range(TOP):
            total = total + weight[:, choice:choice + 1] * y_one[safe_slot[:, choice]].astype(jnp.float32)
        return total.astype(jnp.bfloat16)

    y_out = lax.map(combine, (y_src, flat_slot, gates_src, kept))
    return y_out.reshape(SOURCES * TOKENS, D)
```

```python
import jax
import jax.numpy as jnp
from jax import lax
from jax.experimental import pallas as pl
from jax.experimental.pallas import tpu as pltpu
from jax.sharding import PartitionSpec as P

CAP_NUM = 5
CAP_DEN = 4
MESH = pl.DeviceIdType.MESH
ANY = pl.BlockSpec(memory_space=pl.ANY)
VMEM_LIMIT = 67_043_328


def slot_numbers(expert_ids, n_experts):
    tokens = expert_ids.shape[0]
    expert = jnp.arange(n_experts, dtype=jnp.int32)[:, None]
    chosen = (expert_ids[:, 0][None, :] == expert) | (expert_ids[:, 1][None, :] == expert)
    lane = 128
    blocks = tokens // lane
    bits = chosen.reshape(n_experts, blocks, lane).astype(jnp.bfloat16)
    before = (jnp.arange(lane)[:, None] < jnp.arange(lane)[None, :]).astype(jnp.bfloat16)
    inside = jnp.einsum('ebi,ij->ebj', bits, before, preferred_element_type=jnp.float32)
    totals = jnp.sum(bits.astype(jnp.float32), axis=2).astype(jnp.bfloat16)
    earlier = (jnp.arange(blocks)[:, None] < jnp.arange(blocks)[None, :]).astype(jnp.bfloat16)
    offsets = jnp.einsum('eb,bc->ec', totals, earlier, preferred_element_type=jnp.float32)
    slots = (inside + offsets[:, :, None]).astype(jnp.int32).reshape(n_experts, tokens)
    return chosen, slots


def flip(bit, mask):
    return bit + mask - 2 * bit * mask


def layer_kernel(rows, wg, wu, wd, ret, arrived, bg, bu, bd,
                 xv, gv, uv, dv, hv, acc, yv,
                 x_sem, w_sem, own_sem,
                 disp_s, disp_r, core_s, core_r, y_s, y_r, x_s, x_r, d1_s, d1_r, d2_s, d2_r, ret_s, ret_r):
    dp, z, tp = lax.axis_index('dp'), lax.axis_index('ep'), lax.axis_index('tp')
    y, c = tp // 2, tp % 2
    n_rows = rows.shape[1]
    ff = wg.shape[2]
    n_ep = rows.shape[0]
    n_tp = 4
    w_in, w_buf, w_vmem = (wg, wu, wd), (bg, bu, bd), (gv, uv, dv)

    def partner(k):
        return 2 * flip(z // 2, 1 - k // 2) + flip(z % 2, ((k + 1) // 2) % 2)

    def remote(src, dst, send, recv, device):
        return pltpu.make_async_remote_copy(src_ref=src, dst_ref=dst, send_sem=send, recv_sem=recv,
                                            device_id=device, device_id_type=MESH)

    peer_core = (dp, z, 2 * y + 1 - c)

    def piece(p, half):
        size = w_in[p // 2].shape[1] // 4
        return pl.ds(pl.multiple_of(half * 2 * size + (p % 2) * size, 16), size)

    def core_copy(a):
        return remote(w_in[a].at[y], w_buf[a].at[0], core_s.at[a], core_r.at[a], peer_core)

    def y_copy(p):
        a, at = p // 2, piece(p, dp)
        return remote(w_in[a].at[1 - y, at], w_buf[a].at[1, at], y_s.at[p], y_r.at[p], (dp, z, 2 * (1 - y) + c))

    def x_copy(p):
        a, at = p // 2, piece(p, dp)
        return remote(w_buf[a].at[1, at], w_buf[a].at[1, at], x_s.at[p], x_r.at[p], (1 - dp, z, tp))

    def d1_copy(p):
        a, at = p // 2, piece(p, dp)
        return remote(w_buf[a].at[1, at], w_buf[a].at[2, at], d1_s.at[p], d1_r.at[p], peer_core)

    def d2_copy(p):
        a, at = p // 2, piece(p, 1 - dp)
        return remote(w_buf[a].at[1, at], w_buf[a].at[2, at], d2_s.at[p], d2_r.at[p], peer_core)

    def dispatch(k):
        return remote(rows.at[partner(k)], arrived.at[k], disp_s.at[k], disp_r.at[k], (dp, partner(k), tp))

    def give_back(k, step):
        quarter = (tp + step) % n_tp
        return remote(yv.at[k, quarter], ret.at[z, tp], ret_s.at[k, step], ret_r.at[k, step],
                      (dp, partner(k), quarter))

    def keep_own():
        return pltpu.make_async_copy(yv.at[n_ep - 1, tp], ret.at[z, tp], own_sem)

    def forward_y(p):
        y_copy(p).wait_recv()
        x_copy(p).start()
        d1_copy(p).start()

    def forward_x(p):
        x_copy(p).wait_recv()
        d2_copy(p).start()

    def load_w(slice_no, slot, a):
        src = w_in[a].at[y] if slice_no == 0 else w_buf[a].at[slice_no - 1]
        return pltpu.make_async_copy(src, w_vmem[a].at[slot], w_sem.at[slot, a])

    def start_w(slice_no, slot):
        for number in range(4):
            @pl.when(slice_no == number)
            def _():
                for a in range(3):
                    load_w(number, slot, a).start()

    def load_x(src, slot):
        return pltpu.make_async_copy(src, xv.at[slot], x_sem.at[slot])

    for k in range(n_ep - 1):
        dispatch(k).start()
    for a in range(3):
        core_copy(a).start()
    for p in range(6):
        y_copy(p).start()
    start_w(0, 0)
    forward_y(0)
    forward_y(1)
    forward_x(0)
    forward_y(2)
    forward_x(1)
    dispatch(0).wait_recv()
    load_x(arrived.at[0], 0).start()

    def step_body(step, carry):
        k, j = step // 4, step % 4
        slot, x_slot = step % 2, k % 2
        last = 4 * n_ep - 1

        @pl.when(step == 0)
        def _():
            for a in range(3):
                core_copy(a).wait_recv()

        @pl.when(step == 2)
        def _():
            for p in range(6):
                d1_copy(p).wait_recv()
                d2_copy(p).wait_recv()

        @pl.when((step != 1) & (step < last))
        def _():
            start_w((j + 1) % 4, 1 - slot)

        @pl.when(j == 0)
        def _():
            load_x(arrived.at[0], x_slot).wait()

        @pl.when((j == 3) & (k < n_ep - 2))
        def _():
            dispatch(k + 1).wait_recv()
            load_x(arrived.at[k + 1], 1 - x_slot).start()

        @pl.when((j == 3) & (k == n_ep - 2))
        def _():
            load_x(rows.at[z], 1 - x_slot).start()

        for a in range(2):
            load_w(0, slot, a).wait()

        def gate_up(at):
            x_now = xv.at[x_slot][...]
            gate = jnp.dot(x_now, gv.at[slot][:, at], preferred_element_type=jnp.float32)
            up = jnp.dot(x_now, uv.at[slot][:, at], preferred_element_type=jnp.float32)
            hv[:, at] = (jax.nn.silu(gate) * up).astype(jnp.bfloat16)

        wide = 256

        def gate_up_loop(t, carry):
            gate_up(pl.ds(pl.multiple_of(t * wide, 128), wide))
            return carry

        lax.fori_loop(0, ff // wide, gate_up_loop, 0)
        if ff % wide:
            gate_up(pl.ds(ff // wide * wide, ff % wide))

        load_w(0, slot, 2).wait()
        quarter_cols = ret.shape[3]

        def down_loop(q, carry):
            at = pl.ds(pl.multiple_of(q * quarter_cols, 128), quarter_cols)
            part = jnp.dot(hv[...], dv.at[slot][:, at], preferred_element_type=jnp.float32)

            @pl.when(j == 0)
            def _():
                acc.at[q][...] = part

            @pl.when((j > 0) & (j < 3))
            def _():
                acc.at[q][...] += part

            @pl.when(j == 3)
            def _():
                yv.at[k, q][...] = (acc.at[q][...] + part).astype(jnp.bfloat16)
            return carry

        lax.fori_loop(0, n_tp, down_loop, 0)

        @pl.when(step == 0)
        def _():
            forward_y(3)
            forward_x(2)

        @pl.when(step == 1)
        def _():
            forward_y(4)
            forward_x(3)
            forward_y(5)
            forward_x(4)
            forward_x(5)
            start_w(2, 1 - slot)

        @pl.when((j == 3) & (k < n_ep - 1))
        def _():
            for q in range(n_tp):
                give_back(k, q).start()
        return carry

    lax.fori_loop(0, 4 * n_ep, step_body, 0)
    keep_own().start()
    for q in range(1, n_tp):
        give_back(n_ep - 1, q).start()

    for k in range(n_ep - 1):
        dispatch(k).wait_send()
    for a in range(3):
        core_copy(a).wait_send()
    for p in range(6):
        y_copy(p).wait_send()
        x_copy(p).wait_send()
        d1_copy(p).wait_send()
        d2_copy(p).wait_send()
    keep_own().wait()
    for k in range(n_ep):
        for q in range(n_tp):
            if k == n_ep - 1 and q == 0:
                continue
            give_back(k, q).wait_send()
    for k in range(n_ep):
        for q in range(n_tp):
            if k == n_ep - 1 and q == 0:
                continue
            source = (tp + n_tp - q) % n_tp
            remote(yv.at[k, source], ret.at[partner(k), source], ret_s.at[k, q], ret_r.at[k, q],
                   (dp, partner(k), source)).wait_recv()


def run_layer(rows, wg, wu, wd):
    n_ep, n_rows, d_model = rows.shape
    ff = wg.shape[2]
    quarter = d_model // 4
    bf16, dma = jnp.bfloat16, pltpu.SemaphoreType.DMA
    outs = pl.pallas_call(
        layer_kernel,
        name='moe_layer',
        out_shape=[jax.ShapeDtypeStruct((n_ep, 4, n_rows, quarter), bf16),
                   jax.ShapeDtypeStruct((n_ep - 1, n_rows, d_model), bf16),
                   jax.ShapeDtypeStruct((3, d_model, ff), bf16),
                   jax.ShapeDtypeStruct((3, d_model, ff), bf16),
                   jax.ShapeDtypeStruct((3, ff, d_model), bf16)],
        in_specs=[ANY] * 4,
        out_specs=[ANY] * 5,
        scratch_shapes=[pltpu.VMEM((2, n_rows, d_model), bf16),
                        pltpu.VMEM((2, d_model, ff), bf16),
                        pltpu.VMEM((2, d_model, ff), bf16),
                        pltpu.VMEM((2, ff, d_model), bf16),
                        pltpu.VMEM((n_rows, ff), bf16),
                        pltpu.VMEM((4, n_rows, quarter), jnp.float32),
                        pltpu.VMEM((n_ep, 4, n_rows, quarter), bf16),
                        dma((2,)), dma((2, 3)), dma,
                        dma((n_ep - 1,)), dma((n_ep - 1,)), dma((3,)), dma((3,)),
                        dma((6,)), dma((6,)), dma((6,)), dma((6,)),
                        dma((6,)), dma((6,)), dma((6,)), dma((6,)),
                        dma((n_ep, 4)), dma((n_ep, 4))],
        compiler_params=pltpu.CompilerParams(has_side_effects=True, vmem_limit_bytes=VMEM_LIMIT),
    )(rows, wg, wu, wd)
    return outs[0]


def combine_kernel(first, second, gate0, gate1, results, out, wide, tile):
    n_res = results.shape[0]
    tokens = out.shape[0]
    block = n_res // 16

    def widen(r, carry):
        at = pl.ds(pl.multiple_of(r * block, 8), block)
        wide[at, :] = results[at, :].astype(jnp.float32)
        return carry

    lax.fori_loop(0, 16, widen, 0)
    wide[pl.ds(n_res, 8), :] = jnp.zeros((8, wide.shape[1]), jnp.float32)
    chunk = tile.shape[0]

    def chunk_body(b, carry):
        def eight(i, carry):
            for u in range(8):
                local = i * 8 + u
                t = b * chunk + local
                row = gate0[t] * wide[pl.ds(first[t], 1), :] + gate1[t] * wide[pl.ds(second[t], 1), :]
                tile[pl.ds(local, 1), :] = row
            return carry

        lax.fori_loop(0, chunk // 8, eight, 0)
        out[pl.ds(pl.multiple_of(b * chunk, 8), chunk), :] = tile[...].astype(jnp.bfloat16)
        return carry

    lax.fori_loop(0, tokens // chunk, chunk_body, 0)


def run_combine(index, gates, results):
    tokens = index.shape[1]
    cols = results.shape[1]
    smem = pl.BlockSpec(memory_space=pltpu.SMEM)
    vmem = pl.BlockSpec(memory_space=pltpu.VMEM)
    return pl.pallas_call(
        combine_kernel,
        name='moe_combine',
        out_shape=jax.ShapeDtypeStruct((tokens, cols), jnp.bfloat16),
        in_specs=[smem] * 4 + [vmem],
        out_specs=vmem,
        scratch_shapes=[pltpu.VMEM((results.shape[0] + 8, cols), jnp.float32),
                        pltpu.VMEM((min(256, tokens), cols), jnp.float32)],
        compiler_params=pltpu.CompilerParams(vmem_limit_bytes=VMEM_LIMIT),
    )(index[0], index[1], gates[0], gates[1], results)


def solution(mesh):
    n_ep = mesh.shape['ep']
    row_spec = P(('dp', 'ep'), None)

    def device_body(x_loc, ids_loc, gates_loc, wg_loc, wu_loc, wd_loc):
        tokens, d_model = x_loc.shape
        n_top = ids_loc.shape[1]
        local_experts = wg_loc.shape[0]
        n_experts = local_experts * n_ep
        capacity = CAP_NUM * n_top * tokens // (CAP_DEN * n_experts)
        half = capacity // 2
        tp = lax.axis_index('tp')
        parity, part = tp // 2, tp % 2
        chosen, slots = slot_numbers(ids_loc, n_experts)
        taken = jnp.where(chosen, slots, -1).reshape(n_ep, local_experts, tokens)
        taken = lax.dynamic_index_in_dim(taken, parity, axis=1, keepdims=False)
        wanted = part * half + jnp.arange(half, dtype=jnp.int32)
        number = jnp.arange(tokens, dtype=jnp.int32)
        owner = jnp.max(jnp.where(taken[:, None, :] == wanted[None, :, None], number, 0), axis=2)
        rows = jnp.take(x_loc, owner, axis=0, mode='clip')
        ids_t = ids_loc.T
        expert = jnp.arange(n_experts, dtype=jnp.int32)[None, :, None]
        copy_slot = jnp.sum(jnp.where(ids_t[:, None, :] == expert, slots[None], 0), axis=1)
        index = jnp.where(copy_slot < capacity, ids_t * capacity + copy_slot, n_experts * capacity)
        results = run_layer(rows, wg_loc, wu_loc, wd_loc)
        results = results.reshape(n_experts * capacity, d_model // 4)
        mine = run_combine(index, gates_loc.T, results)
        return lax.all_gather(mine, 'tp', axis=1, tiled=True)

    return jax.shard_map(device_body, mesh=mesh,
                         in_specs=(row_spec, row_spec, row_spec, P('ep', None, 'tp'), P('ep', None, 'tp'), P('ep', 'tp', None)),
                         out_specs=row_spec, check_vma=False)
```

```python
import jax
import jax.numpy as jnp
from jax import lax
from jax.experimental import pallas as pl
from jax.experimental.pallas import tpu as pltpu
from jax.sharding import PartitionSpec as P

CAP_NUM = 5
CAP_DEN = 4
MESH = pl.DeviceIdType.MESH
SUBS = 4
PIECES = 3 * SUBS
AHEAD = 2
ANY = pl.BlockSpec(memory_space=pl.ANY)
VMEM_LIMIT = 67_043_328


def slot_numbers(expert_ids, n_experts):
    tokens = expert_ids.shape[0]
    expert = jnp.arange(n_experts, dtype=jnp.int32)[:, None]
    chosen = (expert_ids[:, 0][None, :] == expert) | (expert_ids[:, 1][None, :] == expert)
    lane = 128
    blocks = tokens // lane
    bits = chosen.reshape(n_experts, blocks, lane).astype(jnp.bfloat16)
    before = (jnp.arange(lane)[:, None] < jnp.arange(lane)[None, :]).astype(jnp.bfloat16)
    inside = jnp.einsum('ebi,ij->ebj', bits, before, preferred_element_type=jnp.float32)
    totals = jnp.sum(bits.astype(jnp.float32), axis=2).astype(jnp.bfloat16)
    earlier = (jnp.arange(blocks)[:, None] < jnp.arange(blocks)[None, :]).astype(jnp.bfloat16)
    offsets = jnp.einsum('eb,bc->ec', totals, earlier, preferred_element_type=jnp.float32)
    slots = (inside + offsets[:, :, None]).astype(jnp.int32).reshape(n_experts, tokens)
    return chosen, slots


def flip(bit, mask):
    return bit + mask - 2 * bit * mask


def layer_kernel(rows, wg, wu, wd, ret, arrived, bg, bu, bd,
                 xv, gv, uv, dv, hv, acc, yv,
                 x_sem, w_sem, own_sem,
                 disp_s, disp_r, core_s, core_r, y_s, y_r, x_s, x_r, d1_s, d1_r, d2_s, d2_r, ret_s, ret_r):
    dp, z, tp = lax.axis_index('dp'), lax.axis_index('ep'), lax.axis_index('tp')
    y, c = tp // 2, tp % 2
    n_rows = rows.shape[1]
    ff = wg.shape[2]
    n_ep = rows.shape[0]
    n_tp = 4
    w_in, w_buf, w_vmem = (wg, wu, wd), (bg, bu, bd), (gv, uv, dv)

    def partner(k):
        return 2 * flip(z // 2, 1 - k // 2) + flip(z % 2, ((k + 1) // 2) % 2)

    def remote(src, dst, send, recv, device):
        return pltpu.make_async_remote_copy(src_ref=src, dst_ref=dst, send_sem=send, recv_sem=recv,
                                            device_id=device, device_id_type=MESH)

    peer_core = (dp, z, 2 * y + 1 - c)

    def piece(p, half):
        size = w_in[p // SUBS].shape[1] // (2 * SUBS)
        return pl.ds(pl.multiple_of((half * SUBS + p % SUBS) * size, 16), size)

    def core_copy(a):
        return remote(w_in[a].at[y], w_buf[a].at[0], core_s.at[a], core_r.at[a], peer_core)

    def y_copy(p):
        a, at = p // SUBS, piece(p, dp)
        return remote(w_in[a].at[1 - y, at], w_buf[a].at[1, at], y_s.at[p], y_r.at[p], (dp, z, 2 * (1 - y) + c))

    def x_copy(p):
        a, at = p // SUBS, piece(p, dp)
        return remote(w_buf[a].at[1, at], w_buf[a].at[1, at], x_s.at[p], x_r.at[p], (1 - dp, z, tp))

    def d1_copy(p):
        a, at = p // SUBS, piece(p, dp)
        return remote(w_buf[a].at[1, at], w_buf[a].at[2, at], d1_s.at[p], d1_r.at[p], peer_core)

    def d2_copy(p):
        a, at = p // SUBS, piece(p, 1 - dp)
        return remote(w_buf[a].at[1, at], w_buf[a].at[2, at], d2_s.at[p], d2_r.at[p], peer_core)

    def dispatch(k):
        return remote(rows.at[partner(k)], arrived.at[k], disp_s.at[k], disp_r.at[k], (dp, partner(k), tp))

    def give_back(k, step):
        quarter = (tp + step) % n_tp
        return remote(yv.at[k, quarter], ret.at[z, tp], ret_s.at[k, step], ret_r.at[k, step],
                      (dp, partner(k), quarter))

    def keep_own():
        return pltpu.make_async_copy(yv.at[n_ep - 1, tp], ret.at[z, tp], own_sem)

    def forward_y(p):
        y_copy(p).wait_recv()
        x_copy(p).start()
        d1_copy(p).start()
        if p + AHEAD < PIECES:
            y_copy(p).wait_send()
            y_copy(p + AHEAD).start()

    def forward_x(p):
        x_copy(p).wait_recv()
        d2_copy(p).start()

    def load_w(slice_no, slot, a):
        src = w_in[a].at[y] if slice_no == 0 else w_buf[a].at[slice_no - 1]
        return pltpu.make_async_copy(src, w_vmem[a].at[slot], w_sem.at[slot, a])

    def start_w(slice_no, slot):
        for number in range(4):
            @pl.when(slice_no == number)
            def _():
                for a in range(3):
                    load_w(number, slot, a).start()

    def load_x(src, slot):
        return pltpu.make_async_copy(src, xv.at[slot], x_sem.at[slot])

    dispatch(0).start()
    for p in range(AHEAD):
        y_copy(p).start()
    for a in range(3):
        core_copy(a).start()
    start_w(0, 0)
    for p in range(6):
        forward_y(p)
        if p >= 2:
            forward_x(p - 2)
    dispatch(0).wait_recv()
    for k in range(1, n_ep - 1):
        dispatch(k).start()
    load_x(arrived.at[0], 0).start()

    def step_body(step, carry):
        k, j = step // 4, step % 4
        slot, x_slot = step % 2, k % 2
        last = 4 * n_ep - 1

        @pl.when(step == 0)
        def _():
            for a in range(3):
                core_copy(a).wait_recv()

        @pl.when(step == 2)
        def _():
            for p in range(PIECES):
                d1_copy(p).wait_recv()
                d2_copy(p).wait_recv()

        @pl.when((step != 1) & (step < last))
        def _():
            start_w((j + 1) % 4, 1 - slot)

        @pl.when(j == 0)
        def _():
            load_x(arrived.at[0], x_slot).wait()

        @pl.when((j == 3) & (k < n_ep - 2))
        def _():
            dispatch(k + 1).wait_recv()
            load_x(arrived.at[k + 1], 1 - x_slot).start()

        @pl.when((j == 3) & (k == n_ep - 2))
        def _():
            load_x(rows.at[z], 1 - x_slot).start()

        for a in range(2):
            load_w(0, slot, a).wait()

        def gate_up(at):
            x_now = xv.at[x_slot][...]
            gate = jnp.dot(x_now, gv.at[slot][:, at], preferred_element_type=jnp.float32)
            up = jnp.dot(x_now, uv.at[slot][:, at], preferred_element_type=jnp.float32)
            hv[:, at] = (jax.nn.silu(gate) * up).astype(jnp.bfloat16)

        wide = 256

        def gate_up_loop(t, carry):
            gate_up(pl.ds(pl.multiple_of(t * wide, 128), wide))
            return carry

        lax.fori_loop(0, ff // wide, gate_up_loop, 0)
        if ff % wide:
            gate_up(pl.ds(ff // wide * wide, ff % wide))

        load_w(0, slot, 2).wait()
        quarter_cols = ret.shape[3]

        def down_loop(q, carry):
            at = pl.ds(pl.multiple_of(q * quarter_cols, 128), quarter_cols)
            part = jnp.dot(hv[...], dv.at[slot][:, at], preferred_element_type=jnp.float32)

            @pl.when(j == 0)
            def _():
                acc.at[q][...] = part

            @pl.when((j > 0) & (j < 3))
            def _():
                acc.at[q][...] += part

            @pl.when(j == 3)
            def _():
                yv.at[k, q][...] = (acc.at[q][...] + part).astype(jnp.bfloat16)
            return carry

        lax.fori_loop(0, n_tp, down_loop, 0)

        @pl.when(step == 0)
        def _():
            for p in range(6, 8):
                forward_y(p)
                forward_x(p - 2)

        @pl.when(step == 1)
        def _():
            for p in range(8, PIECES):
                forward_y(p)
                forward_x(p - 2)
            for p in range(PIECES - 2, PIECES):
                forward_x(p)
            start_w(2, 1 - slot)

        @pl.when((j == 3) & (k < n_ep - 1))
        def _():
            for q in range(n_tp):
                give_back(k, q).start()
        return carry

    lax.fori_loop(0, 4 * n_ep, step_body, 0)
    keep_own().start()
    for q in range(1, n_tp):
        give_back(n_ep - 1, q).start()

    for k in range(n_ep - 1):
        dispatch(k).wait_send()
    for a in range(3):
        core_copy(a).wait_send()
    for p in range(PIECES):
        if p + AHEAD >= PIECES:
            y_copy(p).wait_send()
        x_copy(p).wait_send()
        d1_copy(p).wait_send()
        d2_copy(p).wait_send()
    keep_own().wait()
    for k in range(n_ep):
        for q in range(n_tp):
            if k == n_ep - 1 and q == 0:
                continue
            give_back(k, q).wait_send()
    for k in range(n_ep):
        for q in range(n_tp):
            if k == n_ep - 1 and q == 0:
                continue
            source = (tp + n_tp - q) % n_tp
            remote(yv.at[k, source], ret.at[partner(k), source], ret_s.at[k, q], ret_r.at[k, q],
                   (dp, partner(k), source)).wait_recv()


def run_layer(rows, wg, wu, wd):
    n_ep, n_rows, d_model = rows.shape
    ff = wg.shape[2]
    quarter = d_model // 4
    bf16, dma = jnp.bfloat16, pltpu.SemaphoreType.DMA
    outs = pl.pallas_call(
        layer_kernel,
        name='moe_layer',
        out_shape=[jax.ShapeDtypeStruct((n_ep, 4, n_rows, quarter), bf16),
                   jax.ShapeDtypeStruct((n_ep - 1, n_rows, d_model), bf16),
                   jax.ShapeDtypeStruct((3, d_model, ff), bf16),
                   jax.ShapeDtypeStruct((3, d_model, ff), bf16),
                   jax.ShapeDtypeStruct((3, ff, d_model), bf16)],
        in_specs=[ANY] * 4,
        out_specs=[ANY] * 5,
        scratch_shapes=[pltpu.VMEM((2, n_rows, d_model), bf16),
                        pltpu.VMEM((2, d_model, ff), bf16),
                        pltpu.VMEM((2, d_model, ff), bf16),
                        pltpu.VMEM((2, ff, d_model), bf16),
                        pltpu.VMEM((n_rows, ff), bf16),
                        pltpu.VMEM((4, n_rows, quarter), jnp.float32),
                        pltpu.VMEM((n_ep, 4, n_rows, quarter), bf16),
                        dma((2,)), dma((2, 3)), dma,
                        dma((n_ep - 1,)), dma((n_ep - 1,)), dma((3,)), dma((3,)),
                        *[dma((PIECES,)) for _ in range(8)],
                        dma((n_ep, 4)), dma((n_ep, 4))],
        compiler_params=pltpu.CompilerParams(has_side_effects=True, vmem_limit_bytes=VMEM_LIMIT),
    )(rows, wg, wu, wd)
    return outs[0]


CHUNKS = 8


def combine_kernel(first, second, gate0, gate1, results, out, wide, tile, done,
                   own_s, core_s, core_r, y_s, y_r, fwd_s, fwd_r):
    dp, z, tp = lax.axis_index('dp'), lax.axis_index('ep'), lax.axis_index('tp')
    y, c = tp // 2, tp % 2
    n_res, cols = results.shape
    chunk = done.shape[1]
    peer_core, peer_chip = 2 * y + 1 - c, 2 * (1 - y) + c

    def place(b, quarter):
        return out.at[pl.ds(pl.multiple_of(b * chunk, 16), chunk), pl.ds(pl.multiple_of(quarter * cols, 128), cols)]

    def remote(src, dst, send, recv, device):
        return pltpu.make_async_remote_copy(src_ref=src, dst_ref=dst, send_sem=send, recv_sem=recv,
                                            device_id=(dp, z, device), device_id_type=MESH)

    def own(b):
        return pltpu.make_async_copy(done.at[b], place(b, tp), own_s.at[b])

    def to_core(b):
        return remote(done.at[b], place(b, tp), core_s.at[b], core_r.at[b], peer_core)

    def to_chip(b):
        return remote(done.at[b], place(b, tp), y_s.at[b], y_r.at[b], peer_chip)

    def forward(b):
        return remote(place(b, peer_chip), place(b, peer_chip), fwd_s.at[b], fwd_r.at[b], peer_core)

    block = n_res // 16

    def widen(r, carry):
        at = pl.ds(pl.multiple_of(r * block, 8), block)
        wide[at, :] = results[at, :].astype(jnp.float32)
        return carry

    lax.fori_loop(0, 16, widen, 0)
    wide[pl.ds(n_res, 8), :] = jnp.zeros((8, cols), jnp.float32)
    part = tile.shape[0]

    def part_body(i, carry):
        def eight(g, carry):
            for u in range(8):
                local = g * 8 + u
                t = i * part + local
                row = gate0[t] * wide[pl.ds(first[t], 1), :] + gate1[t] * wide[pl.ds(second[t], 1), :]
                tile[pl.ds(local, 1), :] = row
            return carry

        lax.fori_loop(0, part // 8, eight, 0)
        per = chunk // part
        b = i // per
        done[b, pl.ds(pl.multiple_of(i % per * part, 16), part), :] = tile[...].astype(jnp.bfloat16)

        @pl.when(i % per == per - 1)
        def _():
            to_chip(b).start()
            to_core(b).start()
            own(b).start()
        return carry

    lax.fori_loop(0, CHUNKS * chunk // part, part_body, 0)
    for b in range(CHUNKS):
        to_chip(b).wait_recv()
        forward(b).start()
    for b in range(CHUNKS):
        own(b).wait()
        to_chip(b).wait_send()
        to_core(b).wait_send()
        forward(b).wait_send()
        to_core(b).wait_recv()
        forward(b).wait_recv()


def run_combine(index, gates, results):
    tokens = index.shape[1]
    cols = results.shape[1]
    chunk = tokens // CHUNKS
    bf16, dma = jnp.bfloat16, pltpu.SemaphoreType.DMA
    smem = pl.BlockSpec(memory_space=pltpu.SMEM)
    vmem = pl.BlockSpec(memory_space=pltpu.VMEM)
    return pl.pallas_call(
        combine_kernel,
        name='moe_combine',
        out_shape=jax.ShapeDtypeStruct((tokens, 4 * cols), bf16),
        in_specs=[smem] * 4 + [vmem],
        out_specs=ANY,
        scratch_shapes=[pltpu.VMEM((results.shape[0] + 8, cols), jnp.float32),
                        pltpu.VMEM((min(256, chunk), cols), jnp.float32),
                        pltpu.VMEM((CHUNKS, chunk, cols), bf16),
                        *[dma((CHUNKS,)) for _ in range(7)]],
        compiler_params=pltpu.CompilerParams(has_side_effects=True, vmem_limit_bytes=VMEM_LIMIT),
    )(index[0], index[1], gates[0], gates[1], results)


def solution(mesh):
    n_ep = mesh.shape['ep']
    row_spec = P(('dp', 'ep'), None)

    def device_body(x_loc, ids_loc, gates_loc, wg_loc, wu_loc, wd_loc):
        tokens, d_model = x_loc.shape
        n_top = ids_loc.shape[1]
        local_experts = wg_loc.shape[0]
        n_experts = local_experts * n_ep
        capacity = CAP_NUM * n_top * tokens // (CAP_DEN * n_experts)
        half = capacity // 2
        tp = lax.axis_index('tp')
        parity, part = tp // 2, tp % 2
        chosen, slots = slot_numbers(ids_loc, n_experts)
        taken = jnp.where(chosen, slots, -1).reshape(n_ep, local_experts, tokens)
        taken = lax.dynamic_index_in_dim(taken, parity, axis=1, keepdims=False)
        wanted = part * half + jnp.arange(half, dtype=jnp.int32)
        number = jnp.arange(tokens, dtype=jnp.int32)
        owner = jnp.max(jnp.where(taken[:, None, :] == wanted[None, :, None], number, 0), axis=2)
        rows = jnp.take(x_loc, owner, axis=0, mode='clip')
        ids_t = ids_loc.T
        expert = jnp.arange(n_experts, dtype=jnp.int32)[None, :, None]
        copy_slot = jnp.sum(jnp.where(ids_t[:, None, :] == expert, slots[None], 0), axis=1)
        index = jnp.where(copy_slot < capacity, ids_t * capacity + copy_slot, n_experts * capacity)
        results = run_layer(rows, wg_loc, wu_loc, wd_loc)
        results = results.reshape(n_experts * capacity, d_model // 4)
        return run_combine(index, gates_loc.T, results)

    return jax.shard_map(device_body, mesh=mesh,
                         in_specs=(row_spec, row_spec, row_spec, P('ep', None, 'tp'), P('ep', None, 'tp'), P('ep', 'tp', None)),
                         out_specs=row_spec, check_vma=False)
```

```python
import jax
import jax.numpy as jnp
from jax import lax
from jax.experimental import pallas as pl
from jax.experimental.pallas import tpu as pltpu
from jax.sharding import PartitionSpec as P

CAP_NUM = 5
CAP_DEN = 4
MESH = pl.DeviceIdType.MESH
SUBS = 4
PIECES = 3 * SUBS
AHEAD = 2
ANY = pl.BlockSpec(memory_space=pl.ANY)
VMEM_LIMIT = 67_043_328


def slot_numbers(expert_ids, n_experts):
    tokens = expert_ids.shape[0]
    expert = jnp.arange(n_experts, dtype=jnp.int32)[:, None]
    chosen = (expert_ids[:, 0][None, :] == expert) | (expert_ids[:, 1][None, :] == expert)
    lane = 128
    blocks = tokens // lane
    bits = chosen.reshape(n_experts, blocks, lane).astype(jnp.bfloat16)
    before = (jnp.arange(lane)[:, None] < jnp.arange(lane)[None, :]).astype(jnp.bfloat16)
    inside = jnp.einsum('ebi,ij->ebj', bits, before, preferred_element_type=jnp.float32)
    totals = jnp.sum(bits.astype(jnp.float32), axis=2).astype(jnp.bfloat16)
    earlier = (jnp.arange(blocks)[:, None] < jnp.arange(blocks)[None, :]).astype(jnp.bfloat16)
    offsets = jnp.einsum('eb,bc->ec', totals, earlier, preferred_element_type=jnp.float32)
    slots = (inside + offsets[:, :, None]).astype(jnp.int32).reshape(n_experts, tokens)
    return chosen, slots


def flip(bit, mask):
    return bit + mask - 2 * bit * mask


def layer_kernel(taken, x, wg, wu, wd, ret, rows, arrived, bg, bu, bd,
                 xv, gv, uv, dv, hv, acc, yv,
                 x_sem, w_sem, own_sem, row_sem,
                 first_s, first_r, disp_s, disp_r, core_s, core_r, y_s, y_r, x_s, x_r, d1_s, d1_r, d2_s, d2_r, ret_s, ret_r):
    dp, z, tp = lax.axis_index('dp'), lax.axis_index('ep'), lax.axis_index('tp')
    y, c = tp // 2, tp % 2
    n_rows = rows.shape[1]
    ff = wg.shape[2]
    n_ep = rows.shape[0]
    n_tp = 4
    w_in, w_buf, w_vmem = (wg, wu, wd), (bg, bu, bd), (gv, uv, dv)

    def partner(k):
        return 2 * flip(z // 2, 1 - k // 2) + flip(z % 2, ((k + 1) // 2) % 2)

    def remote(src, dst, send, recv, device):
        return pltpu.make_async_remote_copy(src_ref=src, dst_ref=dst, send_sem=send, recv_sem=recv,
                                            device_id=device, device_id_type=MESH)

    peer_core = (dp, z, 2 * y + 1 - c)

    def piece(p, half):
        size = w_in[p // SUBS].shape[1] // (2 * SUBS)
        return pl.ds(pl.multiple_of((half * SUBS + p % SUBS) * size, 16), size)

    def core_copy(a):
        return remote(w_in[a].at[y], w_buf[a].at[0], core_s.at[a], core_r.at[a], peer_core)

    def y_copy(p):
        a, at = p // SUBS, piece(p, dp)
        return remote(w_in[a].at[1 - y, at], w_buf[a].at[1, at], y_s.at[p], y_r.at[p], (dp, z, 2 * (1 - y) + c))

    def x_copy(p):
        a, at = p // SUBS, piece(p, dp)
        return remote(w_buf[a].at[1, at], w_buf[a].at[1, at], x_s.at[p], x_r.at[p], (1 - dp, z, tp))

    def d1_copy(p):
        a, at = p // SUBS, piece(p, dp)
        return remote(w_buf[a].at[1, at], w_buf[a].at[2, at], d1_s.at[p], d1_r.at[p], peer_core)

    def d2_copy(p):
        a, at = p // SUBS, piece(p, 1 - dp)
        return remote(w_buf[a].at[1, at], w_buf[a].at[2, at], d2_s.at[p], d2_r.at[p], peer_core)

    def dispatch(k):
        return remote(rows.at[k], arrived.at[k], disp_s.at[k], disp_r.at[k], (dp, partner(k), tp))

    def dispatch_first(q):
        cols = pl.ds(pl.multiple_of(q * ret.shape[3], 128), ret.shape[3])
        return remote(rows.at[0, :, cols], arrived.at[0, :, cols], first_s.at[q], first_r.at[q], (dp, partner(0), tp))

    def give_back(k, step):
        quarter = (tp + step) % n_tp
        return remote(yv.at[k, quarter], ret.at[z, tp], ret_s.at[k, step], ret_r.at[k, step],
                      (dp, partner(k), quarter))

    def keep_own():
        return pltpu.make_async_copy(yv.at[n_ep - 1, tp], ret.at[z, tp], own_sem)

    def forward_y(p):
        y_copy(p).wait_recv()
        x_copy(p).start()
        d1_copy(p).start()
        if p + AHEAD < PIECES:
            y_copy(p).wait_send()
            y_copy(p + AHEAD).start()

    def forward_x(p):
        x_copy(p).wait_recv()
        d2_copy(p).start()

    def load_w(slice_no, slot, a):
        src = w_in[a].at[y] if slice_no == 0 else w_buf[a].at[slice_no - 1]
        return pltpu.make_async_copy(src, w_vmem[a].at[slot], w_sem.at[slot, a])

    def start_w(slice_no, slot):
        for number in range(4):
            @pl.when(slice_no == number)
            def _():
                for a in range(3):
                    load_w(number, slot, a).start()

    def load_x(src, slot):
        return pltpu.make_async_copy(src, xv.at[slot], x_sem.at[slot])

    for p in range(AHEAD):
        y_copy(p).start()
    for a in range(3):
        core_copy(a).start()

    tokens, d_model = x.shape
    half_t, half_d = tokens // 2, d_model // 2
    quarter_cols = ret.shape[3]

    def load_tokens(h, side):
        return pltpu.make_async_copy(x.at[pl.ds(h * half_t, half_t), pl.ds(side * half_d, half_d)],
                                     w_vmem[h].at[side, pl.ds(0, half_t), pl.ds(0, half_d)], w_sem.at[side, h])

    def store_rows(k, q):
        cols = pl.ds(pl.multiple_of(q * quarter_cols, 128), quarter_cols)
        return pltpu.make_async_copy(yv.at[k, q], rows.at[k, :, cols], row_sem.at[q])

    for side in range(2):
        for h in range(2):
            load_tokens(h, side).start()

    def pick_rows(k, carry):
        wanted = lax.broadcasted_iota(jnp.int32, (n_rows, 128), 0) + c * n_rows
        for h in range(2):
            def mark(t, carry):
                at = pl.multiple_of(t * 128, 128)
                owned = taken.at[partner(k)][pl.ds(h * (half_t // 128) + t, 1), :]
                xv.at[h][:, pl.ds(at, 128)] = jnp.where(owned == wanted, 1.0, 0.0).astype(jnp.bfloat16)
                return carry

            lax.fori_loop(0, half_t // 128, mark, 0)

        @pl.when(k == 0)
        def _():
            for side in range(2):
                for h in range(2):
                    load_tokens(h, side).wait()

        def pick_cols(q, carry):
            at = pl.ds(pl.multiple_of(q % 2 * quarter_cols, 128), quarter_cols)
            picked = [jnp.dot(xv.at[h][:, pl.ds(0, half_t)], w_vmem[h].at[q // 2][pl.ds(0, half_t), at],
                              preferred_element_type=jnp.float32) for h in range(2)]
            yv.at[k, q][...] = (picked[0] + picked[1]).astype(jnp.bfloat16)
            store_rows(k, q).start()

            @pl.when(k == 0)
            def _():
                store_rows(k, q).wait()
                dispatch_first(q).start()
            return carry

        lax.fori_loop(0, n_tp, pick_cols, 0)

        @pl.when(k > 0)
        def _():
            for q in range(n_tp):
                store_rows(k, q).wait()

        @pl.when(k == 2)
        def _():
            for p in range(2):
                forward_y(p)
        return carry

    lax.fori_loop(0, n_ep, pick_rows, 0)
    start_w(0, 0)
    for p in range(2, 6):
        forward_y(p)
        forward_x(p - 2)
    for q in range(n_tp):
        dispatch_first(q).wait_recv()
    for k in range(1, n_ep - 1):
        dispatch(k).start()
    load_x(arrived.at[0], 0).start()

    def gate_up_all(x_slot, slot, h_slot):
        def gate_up(at):
            x_now = xv.at[x_slot][...]
            gate = jnp.dot(x_now, gv.at[slot][:, at], preferred_element_type=jnp.float32)
            up = jnp.dot(x_now, uv.at[slot][:, at], preferred_element_type=jnp.float32)
            hv.at[h_slot][:, at] = (jax.nn.silu(gate) * up).astype(jnp.bfloat16)

        wide = 256

        def gate_up_loop(t, carry):
            gate_up(pl.ds(pl.multiple_of(t * wide, 128), wide))
            return carry

        lax.fori_loop(0, ff // wide, gate_up_loop, 0)
        if ff % wide:
            gate_up(pl.ds(ff // wide * wide, ff % wide))

    def down_all(k, j, slot, h_slot):
        def down_loop(q, carry):
            at = pl.ds(pl.multiple_of(q * quarter_cols, 128), quarter_cols)
            part = jnp.dot(hv.at[h_slot][...], dv.at[slot][:, at], preferred_element_type=jnp.float32)

            @pl.when(j == 0)
            def _():
                acc.at[q][...] = part

            @pl.when((j > 0) & (j < 3))
            def _():
                acc.at[q][...] += part

            @pl.when(j == 3)
            def _():
                yv.at[k, q][...] = (acc.at[q][...] + part).astype(jnp.bfloat16)
            return carry

        lax.fori_loop(0, n_tp, down_loop, 0)

    def step_body(step, carry):
        k, j = step // 4, step % 4
        slot, x_slot = step % 2, k % 2
        last = 4 * n_ep - 1

        @pl.when(step == 0)
        def _():
            for a in range(3):
                core_copy(a).wait_recv()

        @pl.when((step != 1) & (step < last))
        def _():
            start_w((j + 1) % 4, 1 - slot)

        @pl.when(j == 0)
        def _():
            load_x(arrived.at[0], x_slot).wait()

        @pl.when((j == 3) & (k < n_ep - 2))
        def _():
            dispatch(k + 1).wait_recv()
            load_x(arrived.at[k + 1], 1 - x_slot).start()

        @pl.when((j == 3) & (k == n_ep - 2))
        def _():
            load_x(rows.at[n_ep - 1], 1 - x_slot).start()

        for a in range(2):
            load_w(0, slot, a).wait()
        gate_up_all(x_slot, slot, 0)
        load_w(0, slot, 2).wait()
        down_all(k, j, slot, 0)

        @pl.when(step == 0)
        def _():
            for p in range(6, 8):
                forward_y(p)
                forward_x(p - 2)

        @pl.when((j == 3) & (k < n_ep - 1))
        def _():
            for q in range(n_tp):
                give_back(k, q).start()
        return carry

    lax.fori_loop(0, 2, step_body, 0)
    gates_done = 2 * SUBS
    for p in range(gates_done, gates_done + 2):
        forward_y(p)
        forward_x(p - 2)
    for a in range(2):
        load_w(2, 0, a).start()
    for p in range(gates_done):
        d1_copy(p).wait_recv()
        d2_copy(p).wait_recv()
    for a in range(2):
        load_w(3, 1, a).start()
    for a in range(2):
        load_w(2, 0, a).wait()
    gate_up_all(0, 0, 0)
    forward_y(gates_done + 2)
    forward_x(gates_done)
    for a in range(2):
        load_w(3, 1, a).wait()
    gate_up_all(0, 1, 1)
    for a in range(2):
        load_w(0, 0, a).start()
    forward_y(gates_done + 3)
    for p in range(gates_done + 1, PIECES):
        forward_x(p)
    load_w(2, 0, 2).start()
    for p in range(gates_done, PIECES):
        d1_copy(p).wait_recv()
        d2_copy(p).wait_recv()
    load_w(3, 1, 2).start()
    load_w(2, 0, 2).wait()
    down_all(0, 2, 0, 0)
    load_w(0, 0, 2).start()
    load_w(3, 1, 2).wait()
    down_all(0, 3, 1, 1)
    for q in range(n_tp):
        give_back(0, q).start()
    dispatch(1).wait_recv()
    load_x(arrived.at[1], 1).start()
    lax.fori_loop(4, 4 * n_ep, step_body, 0)
    keep_own().start()
    for q in range(1, n_tp):
        give_back(n_ep - 1, q).start()

    for q in range(n_tp):
        dispatch_first(q).wait_send()
    for k in range(1, n_ep - 1):
        dispatch(k).wait_send()
    for a in range(3):
        core_copy(a).wait_send()
    for p in range(PIECES):
        if p + AHEAD >= PIECES:
            y_copy(p).wait_send()
        x_copy(p).wait_send()
        d1_copy(p).wait_send()
        d2_copy(p).wait_send()
    keep_own().wait()
    for k in range(n_ep):
        for q in range(n_tp):
            if k == n_ep - 1 and q == 0:
                continue
            give_back(k, q).wait_send()
    for k in range(n_ep):
        for q in range(n_tp):
            if k == n_ep - 1 and q == 0:
                continue
            source = (tp + n_tp - q) % n_tp
            remote(yv.at[k, source], ret.at[partner(k), source], ret_s.at[k, q], ret_r.at[k, q],
                   (dp, partner(k), source)).wait_recv()


def run_layer(taken, x, n_rows, wg, wu, wd):
    n_ep, d_model = taken.shape[0], x.shape[1]
    ff = wg.shape[2]
    quarter = d_model // 4
    bf16, dma = jnp.bfloat16, pltpu.SemaphoreType.DMA
    outs = pl.pallas_call(
        layer_kernel,
        name='moe_layer',
        out_shape=[jax.ShapeDtypeStruct((n_ep, 4, n_rows, quarter), bf16),
                   jax.ShapeDtypeStruct((n_ep, n_rows, d_model), bf16),
                   jax.ShapeDtypeStruct((n_ep - 1, n_rows, d_model), bf16),
                   jax.ShapeDtypeStruct((3, d_model, ff), bf16),
                   jax.ShapeDtypeStruct((3, d_model, ff), bf16),
                   jax.ShapeDtypeStruct((3, ff, d_model), bf16)],
        in_specs=[pl.BlockSpec(memory_space=pltpu.VMEM)] + [ANY] * 4,
        out_specs=[ANY] * 6,
        scratch_shapes=[pltpu.VMEM((2, n_rows, d_model), bf16),
                        pltpu.VMEM((2, d_model, ff), bf16),
                        pltpu.VMEM((2, d_model, ff), bf16),
                        pltpu.VMEM((2, ff, d_model), bf16),
                        pltpu.VMEM((2, n_rows, ff), bf16),
                        pltpu.VMEM((4, n_rows, quarter), jnp.float32),
                        pltpu.VMEM((n_ep, 4, n_rows, quarter), bf16),
                        dma((2,)), dma((2, 3)), dma, dma((4,)), dma((4,)), dma((4,)),
                        dma((n_ep - 1,)), dma((n_ep - 1,)), dma((3,)), dma((3,)),
                        *[dma((PIECES,)) for _ in range(8)],
                        dma((n_ep, 4)), dma((n_ep, 4))],
        compiler_params=pltpu.CompilerParams(has_side_effects=True, vmem_limit_bytes=VMEM_LIMIT),
    )(taken, x, wg, wu, wd)
    return outs[0]


CHUNKS = 8


def combine_kernel(first, second, gates, results, out, wide, tile0, tile1, done,
                   own_s, core_s, core_r, y_s, y_r, fwd_s, fwd_r):
    dp, z, tp = lax.axis_index('dp'), lax.axis_index('ep'), lax.axis_index('tp')
    y, c = tp // 2, tp % 2
    n_res, cols = results.shape
    chunk = done.shape[1]
    peer_core, peer_chip = 2 * y + 1 - c, 2 * (1 - y) + c

    def place(b, quarter):
        return out.at[pl.ds(pl.multiple_of(b * chunk, 16), chunk), pl.ds(pl.multiple_of(quarter * cols, 128), cols)]

    def remote(src, dst, send, recv, device):
        return pltpu.make_async_remote_copy(src_ref=src, dst_ref=dst, send_sem=send, recv_sem=recv,
                                            device_id=(dp, z, device), device_id_type=MESH)

    def own(b):
        return pltpu.make_async_copy(done.at[b], place(b, tp), own_s.at[b])

    def to_core(b):
        return remote(done.at[b], place(b, tp), core_s.at[b], core_r.at[b], peer_core)

    def to_chip(b):
        return remote(done.at[b], place(b, tp), y_s.at[b], y_r.at[b], peer_chip)

    def forward(b):
        return remote(place(b, peer_chip), place(b, peer_chip), fwd_s.at[b], fwd_r.at[b], peer_core)

    block = n_res // 16

    def widen(r, carry):
        at = pl.ds(pl.multiple_of(r * block, 8), block)
        wide[at, :] = results[at, :].astype(jnp.float32)
        return carry

    lax.fori_loop(0, 16, widen, 0)
    wide[pl.ds(n_res, 8), :] = jnp.zeros((8, cols), jnp.float32)
    part = tile0.shape[0]

    def part_body(i, carry):
        def eight(g, carry):
            for u in range(8):
                t = i * part + g * 8 + u
                tile0[pl.ds(g * 8 + u, 1), :] = wide[pl.ds(first[t], 1), :]
                tile1[pl.ds(g * 8 + u, 1), :] = wide[pl.ds(second[t], 1), :]
            return carry

        lax.fori_loop(0, part // 8, eight, 0)
        per = chunk // part
        b = i // per
        weight = gates[pl.ds(pl.multiple_of(i * part, 8), part), :]
        total = weight[:, 0:1] * tile0[...] + weight[:, 1:2] * tile1[...]
        done[b, pl.ds(pl.multiple_of(i % per * part, 16), part), :] = total.astype(jnp.bfloat16)

        @pl.when(i % per == per - 1)
        def _():
            to_chip(b).start()
            to_core(b).start()
            own(b).start()
        return carry

    lax.fori_loop(0, CHUNKS * chunk // part, part_body, 0)
    for b in range(CHUNKS):
        to_chip(b).wait_recv()
        forward(b).start()
    for b in range(CHUNKS):
        own(b).wait()
        to_chip(b).wait_send()
        to_core(b).wait_send()
        forward(b).wait_send()
        to_core(b).wait_recv()
        forward(b).wait_recv()


def run_combine(index, gates, results):
    tokens = index.shape[1]
    cols = results.shape[1]
    chunk = tokens // CHUNKS
    bf16, dma = jnp.bfloat16, pltpu.SemaphoreType.DMA
    smem = pl.BlockSpec(memory_space=pltpu.SMEM)
    vmem = pl.BlockSpec(memory_space=pltpu.VMEM)
    return pl.pallas_call(
        combine_kernel,
        name='moe_combine',
        out_shape=jax.ShapeDtypeStruct((tokens, 4 * cols), bf16),
        in_specs=[smem] * 2 + [vmem] * 2,
        out_specs=ANY,
        scratch_shapes=[pltpu.VMEM((results.shape[0] + 8, cols), jnp.float32),
                        pltpu.VMEM((min(256, chunk), cols), jnp.float32),
                        pltpu.VMEM((min(256, chunk), cols), jnp.float32),
                        pltpu.VMEM((CHUNKS, chunk, cols), bf16),
                        *[dma((CHUNKS,)) for _ in range(7)]],
        compiler_params=pltpu.CompilerParams(has_side_effects=True, vmem_limit_bytes=VMEM_LIMIT),
    )(index[0], index[1], gates, results)


def solution(mesh):
    n_ep = mesh.shape['ep']
    row_spec = P(('dp', 'ep'), None)

    def device_body(x_loc, ids_loc, gates_loc, wg_loc, wu_loc, wd_loc):
        tokens, d_model = x_loc.shape
        n_top = ids_loc.shape[1]
        local_experts = wg_loc.shape[0]
        n_experts = local_experts * n_ep
        capacity = CAP_NUM * n_top * tokens // (CAP_DEN * n_experts)
        parity = lax.axis_index('tp') // 2
        chosen, slots = slot_numbers(ids_loc, n_experts)
        taken = jnp.where(chosen, slots, -1).reshape(n_ep, local_experts, tokens)
        taken = lax.dynamic_index_in_dim(taken, parity, axis=1, keepdims=False)
        ids_t = ids_loc.T
        expert = jnp.arange(n_experts, dtype=jnp.int32)[None, :, None]
        copy_slot = jnp.sum(jnp.where(ids_t[:, None, :] == expert, slots[None], 0), axis=1)
        index = jnp.where(copy_slot < capacity, ids_t * capacity + copy_slot, n_experts * capacity)
        results = run_layer(taken.reshape(n_ep, tokens // 128, 128), x_loc, capacity // 2, wg_loc, wu_loc, wd_loc)
        results = results.reshape(n_experts * capacity, d_model // 4)
        return run_combine(index, gates_loc, results)

    return jax.shard_map(device_body, mesh=mesh,
                         in_specs=(row_spec, row_spec, row_spec, P('ep', None, 'tp'), P('ep', None, 'tp'), P('ep', 'tp', None)),
                         out_specs=row_spec, check_vma=False)
```

```python
import jax
import jax.numpy as jnp
from jax import lax
from jax.experimental import pallas as pl
from jax.experimental.pallas import tpu as pltpu
from jax.sharding import PartitionSpec as P

CAP_NUM = 5
CAP_DEN = 4
MESH = pl.DeviceIdType.MESH
SUBS = 4
PIECES = 3 * SUBS
AHEAD = 2
ANY = pl.BlockSpec(memory_space=pl.ANY)
VMEM_LIMIT = 67_043_328


def slot_numbers(expert_ids, n_experts):
    tokens = expert_ids.shape[0]
    expert = jnp.arange(n_experts, dtype=jnp.int32)[:, None]
    chosen = (expert_ids[:, 0][None, :] == expert) | (expert_ids[:, 1][None, :] == expert)
    lane = 128
    blocks = tokens // lane
    bits = chosen.reshape(n_experts, blocks, lane).astype(jnp.bfloat16)
    before = (jnp.arange(lane)[:, None] < jnp.arange(lane)[None, :]).astype(jnp.bfloat16)
    inside = jnp.einsum('ebi,ij->ebj', bits, before, preferred_element_type=jnp.float32)
    totals = jnp.sum(bits.astype(jnp.float32), axis=2).astype(jnp.bfloat16)
    earlier = (jnp.arange(blocks)[:, None] < jnp.arange(blocks)[None, :]).astype(jnp.bfloat16)
    offsets = jnp.einsum('eb,bc->ec', totals, earlier, preferred_element_type=jnp.float32)
    slots = (inside + offsets[:, :, None]).astype(jnp.int32).reshape(n_experts, tokens)
    return chosen, slots


def flip(bit, mask):
    return bit + mask - 2 * bit * mask


def layer_kernel(taken, x, wg, wu, wd, ret, rows, arrived, bg, bu, bd,
                 xv, gv, uv, dv, hv, acc, yv,
                 x_sem, w_sem, own_sem, row_sem,
                 first_s, first_r, disp_s, disp_r, core_s, core_r, y_s, y_r, x_s, x_r, d1_s, d1_r, d2_s, d2_r, ret_s, ret_r):
    dp, z, tp = lax.axis_index('dp'), lax.axis_index('ep'), lax.axis_index('tp')
    y, c = tp // 2, tp % 2
    n_rows = rows.shape[1]
    ff = wg.shape[2]
    n_ep = rows.shape[0]
    n_tp = 4
    w_in, w_buf, w_vmem = (wg, wu, wd), (bg, bu, bd), (gv, uv, dv)

    def partner(k):
        return 2 * flip(z // 2, 1 - k // 2) + flip(z % 2, ((k + 1) // 2) % 2)

    def remote(src, dst, send, recv, device):
        return pltpu.make_async_remote_copy(src_ref=src, dst_ref=dst, send_sem=send, recv_sem=recv,
                                            device_id=device, device_id_type=MESH)

    peer_core = (dp, z, 2 * y + 1 - c)

    def piece(p, half):
        size = w_in[p // SUBS].shape[1] // (2 * SUBS)
        return pl.ds(pl.multiple_of((half * SUBS + p % SUBS) * size, 16), size)

    def core_copy(a):
        return remote(w_in[a].at[y], w_buf[a].at[0], core_s.at[a], core_r.at[a], peer_core)

    def y_copy(p):
        a, at = p // SUBS, piece(p, dp)
        return remote(w_in[a].at[1 - y, at], w_buf[a].at[1, at], y_s.at[p], y_r.at[p], (dp, z, 2 * (1 - y) + c))

    def x_copy(p):
        a, at = p // SUBS, piece(p, dp)
        return remote(w_buf[a].at[1, at], w_buf[a].at[1, at], x_s.at[p], x_r.at[p], (1 - dp, z, tp))

    def d1_copy(p):
        a, at = p // SUBS, piece(p, dp)
        return remote(w_buf[a].at[1, at], w_buf[a].at[2, at], d1_s.at[p], d1_r.at[p], peer_core)

    def d2_copy(p):
        a, at = p // SUBS, piece(p, 1 - dp)
        return remote(w_buf[a].at[1, at], w_buf[a].at[2, at], d2_s.at[p], d2_r.at[p], peer_core)

    def dispatch(k):
        return remote(rows.at[k], arrived.at[k], disp_s.at[k], disp_r.at[k], (dp, partner(k), tp))

    def dispatch_first(q):
        cols = pl.ds(pl.multiple_of(q * ret.shape[3], 128), ret.shape[3])
        return remote(rows.at[0, :, cols], arrived.at[0, :, cols], first_s.at[q], first_r.at[q], (dp, partner(0), tp))

    def give_back(k, step):
        quarter = (tp + step) % n_tp
        return remote(yv.at[k, quarter], ret.at[z, tp], ret_s.at[k, step], ret_r.at[k, step],
                      (dp, partner(k), quarter))

    def keep_own():
        return pltpu.make_async_copy(yv.at[n_ep - 1, tp], ret.at[z, tp], own_sem)

    def forward_y(p):
        y_copy(p).wait_recv()
        x_copy(p).start()
        d1_copy(p).start()
        if p + AHEAD < PIECES:
            y_copy(p).wait_send()
            y_copy(p + AHEAD).start()

    def forward_x(p):
        x_copy(p).wait_recv()
        d2_copy(p).start()

    def load_w(slice_no, slot, a):
        src = w_in[a].at[y] if slice_no == 0 else w_buf[a].at[slice_no - 1]
        return pltpu.make_async_copy(src, w_vmem[a].at[slot], w_sem.at[slot, a])

    def start_w(slice_no, slot):
        for number in range(4):
            @pl.when(slice_no == number)
            def _():
                for a in range(3):
                    load_w(number, slot, a).start()

    def load_x(src, slot):
        return pltpu.make_async_copy(src, xv.at[slot], x_sem.at[slot])

    for p in range(AHEAD):
        y_copy(p).start()
    for a in range(3):
        core_copy(a).start()

    tokens, d_model = x.shape
    half_t, half_d = tokens // 2, d_model // 2
    quarter_cols = ret.shape[3]

    def load_tokens(h, side):
        return pltpu.make_async_copy(x.at[pl.ds(h * half_t, half_t), pl.ds(side * half_d, half_d)],
                                     w_vmem[h].at[side, pl.ds(0, half_t), pl.ds(0, half_d)], w_sem.at[side, h])

    def store_rows(k, q):
        cols = pl.ds(pl.multiple_of(q * quarter_cols, 128), quarter_cols)
        return pltpu.make_async_copy(yv.at[k, q], rows.at[k, :, cols], row_sem.at[q])

    for side in range(2):
        for h in range(2):
            load_tokens(h, side).start()

    def pick_rows(k, carry):
        wanted = lax.broadcasted_iota(jnp.int32, (n_rows, 128), 0) + c * n_rows
        for h in range(2):
            def mark(t, carry):
                at = pl.multiple_of(t * 128, 128)
                owned = taken.at[partner(k)][pl.ds(h * (half_t // 128) + t, 1), :]
                xv.at[h][:, pl.ds(at, 128)] = jnp.where(owned == wanted, 1.0, 0.0).astype(jnp.bfloat16)
                return carry

            lax.fori_loop(0, half_t // 128, mark, 0)

        def pick_cols(q, carry):
            for side in range(2):
                @pl.when((k == 0) & (q == 2 * side))
                def _():
                    for h in range(2):
                        load_tokens(h, side).wait()

            at = pl.ds(pl.multiple_of(q % 2 * quarter_cols, 128), quarter_cols)
            picked = [jnp.dot(xv.at[h][:, pl.ds(0, half_t)], w_vmem[h].at[q // 2][pl.ds(0, half_t), at],
                              preferred_element_type=jnp.float32) for h in range(2)]
            yv.at[k, q][...] = (picked[0] + picked[1]).astype(jnp.bfloat16)
            store_rows(k, q).start()

            @pl.when(k == 0)
            def _():
                store_rows(k, q).wait()
                dispatch_first(q).start()
            return carry

        lax.fori_loop(0, n_tp, pick_cols, 0)

        @pl.when(k > 0)
        def _():
            for q in range(n_tp):
                store_rows(k, q).wait()

        @pl.when(k == 2)
        def _():
            for p in range(2):
                forward_y(p)
        return carry

    lax.fori_loop(0, n_ep, pick_rows, 0)
    start_w(0, 0)
    for p in range(2, 6):
        forward_y(p)
        forward_x(p - 2)
    for q in range(n_tp):
        dispatch_first(q).wait_recv()
    for k in range(1, n_ep - 1):
        dispatch(k).start()
    load_x(arrived.at[0], 0).start()

    def gate_up_all(x_slot, slot, h_slot):
        def gate_up(at):
            x_now = xv.at[x_slot][...]
            gate = jnp.dot(x_now, gv.at[slot][:, at], preferred_element_type=jnp.float32)
            up = jnp.dot(x_now, uv.at[slot][:, at], preferred_element_type=jnp.float32)
            hv.at[h_slot][:, at] = (jax.nn.silu(gate) * up).astype(jnp.bfloat16)

        wide = 256

        def gate_up_loop(t, carry):
            gate_up(pl.ds(pl.multiple_of(t * wide, 128), wide))
            return carry

        lax.fori_loop(0, ff // wide, gate_up_loop, 0)
        if ff % wide:
            gate_up(pl.ds(ff // wide * wide, ff % wide))

    def down_all(k, j, slot, h_slot):
        def down_loop(q, carry):
            at = pl.ds(pl.multiple_of(q * quarter_cols, 128), quarter_cols)
            part = jnp.dot(hv.at[h_slot][...], dv.at[slot][:, at], preferred_element_type=jnp.float32)

            @pl.when(j == 0)
            def _():
                acc.at[q][...] = part

            @pl.when((j > 0) & (j < 3))
            def _():
                acc.at[q][...] += part

            @pl.when(j == 3)
            def _():
                yv.at[k, q][...] = (acc.at[q][...] + part).astype(jnp.bfloat16)
            return carry

        lax.fori_loop(0, n_tp, down_loop, 0)

    def step_body(step, carry):
        k, j = step // 4, step % 4
        slot, x_slot = step % 2, k % 2
        last = 4 * n_ep - 1

        @pl.when(step == 0)
        def _():
            for a in range(3):
                core_copy(a).wait_recv()

        @pl.when((step != 1) & (step < last))
        def _():
            start_w((j + 1) % 4, 1 - slot)

        @pl.when(j == 0)
        def _():
            load_x(arrived.at[0], x_slot).wait()

        @pl.when((j == 3) & (k < n_ep - 2))
        def _():
            dispatch(k + 1).wait_recv()
            load_x(arrived.at[k + 1], 1 - x_slot).start()

        @pl.when((j == 3) & (k == n_ep - 2))
        def _():
            load_x(rows.at[n_ep - 1], 1 - x_slot).start()

        for a in range(2):
            load_w(0, slot, a).wait()
        gate_up_all(x_slot, slot, 0)
        load_w(0, slot, 2).wait()
        down_all(k, j, slot, 0)

        @pl.when(step == 0)
        def _():
            for p in range(6, 8):
                forward_y(p)
                forward_x(p - 2)

        @pl.when((j == 3) & (k < n_ep - 1))
        def _():
            for q in range(n_tp):
                give_back(k, q).start()
        return carry

    lax.fori_loop(0, 2, step_body, 0)
    gates_done = 2 * SUBS
    for p in range(gates_done, gates_done + 2):
        forward_y(p)
        forward_x(p - 2)
    for a in range(2):
        load_w(2, 0, a).start()
    for p in range(gates_done):
        d1_copy(p).wait_recv()
        d2_copy(p).wait_recv()
    for a in range(2):
        load_w(3, 1, a).start()
    for a in range(2):
        load_w(2, 0, a).wait()
    gate_up_all(0, 0, 0)
    forward_y(gates_done + 2)
    forward_x(gates_done)
    for a in range(2):
        load_w(3, 1, a).wait()
    gate_up_all(0, 1, 1)
    for a in range(2):
        load_w(0, 0, a).start()
    forward_y(gates_done + 3)
    for p in range(gates_done + 1, PIECES):
        forward_x(p)
    load_w(2, 0, 2).start()
    for p in range(gates_done, PIECES):
        d1_copy(p).wait_recv()
        d2_copy(p).wait_recv()
    load_w(3, 1, 2).start()
    load_w(2, 0, 2).wait()
    down_all(0, 2, 0, 0)
    load_w(0, 0, 2).start()
    load_w(3, 1, 2).wait()
    down_all(0, 3, 1, 1)
    for q in range(n_tp):
        give_back(0, q).start()
    dispatch(1).wait_recv()
    load_x(arrived.at[1], 1).start()
    lax.fori_loop(4, 4 * n_ep, step_body, 0)
    keep_own().start()
    for q in range(1, n_tp):
        give_back(n_ep - 1, q).start()

    for q in range(n_tp):
        dispatch_first(q).wait_send()
    for k in range(1, n_ep - 1):
        dispatch(k).wait_send()
    for a in range(3):
        core_copy(a).wait_send()
    for p in range(PIECES):
        if p + AHEAD >= PIECES:
            y_copy(p).wait_send()
        x_copy(p).wait_send()
        d1_copy(p).wait_send()
        d2_copy(p).wait_send()
    keep_own().wait()
    for k in range(n_ep):
        for q in range(n_tp):
            if k == n_ep - 1 and q == 0:
                continue
            give_back(k, q).wait_send()
    for k in range(n_ep):
        for q in range(n_tp):
            if k == n_ep - 1 and q == 0:
                continue
            source = (tp + n_tp - q) % n_tp
            remote(yv.at[k, source], ret.at[partner(k), source], ret_s.at[k, q], ret_r.at[k, q],
                   (dp, partner(k), source)).wait_recv()


def run_layer(taken, x, n_rows, wg, wu, wd):
    n_ep, d_model = taken.shape[0], x.shape[1]
    ff = wg.shape[2]
    quarter = d_model // 4
    bf16, dma = jnp.bfloat16, pltpu.SemaphoreType.DMA
    outs = pl.pallas_call(
        layer_kernel,
        name='moe_layer',
        out_shape=[jax.ShapeDtypeStruct((n_ep, 4, n_rows, quarter), bf16),
                   jax.ShapeDtypeStruct((n_ep, n_rows, d_model), bf16),
                   jax.ShapeDtypeStruct((n_ep - 1, n_rows, d_model), bf16),
                   jax.ShapeDtypeStruct((3, d_model, ff), bf16),
                   jax.ShapeDtypeStruct((3, d_model, ff), bf16),
                   jax.ShapeDtypeStruct((3, ff, d_model), bf16)],
        in_specs=[pl.BlockSpec(memory_space=pltpu.VMEM)] + [ANY] * 4,
        out_specs=[ANY] * 6,
        scratch_shapes=[pltpu.VMEM((2, n_rows, d_model), bf16),
                        pltpu.VMEM((2, d_model, ff), bf16),
                        pltpu.VMEM((2, d_model, ff), bf16),
                        pltpu.VMEM((2, ff, d_model), bf16),
                        pltpu.VMEM((2, n_rows, ff), bf16),
                        pltpu.VMEM((4, n_rows, quarter), jnp.float32),
                        pltpu.VMEM((n_ep, 4, n_rows, quarter), bf16),
                        dma((2,)), dma((2, 3)), dma, dma((4,)), dma((4,)), dma((4,)),
                        dma((n_ep - 1,)), dma((n_ep - 1,)), dma((3,)), dma((3,)),
                        *[dma((PIECES,)) for _ in range(8)],
                        dma((n_ep, 4)), dma((n_ep, 4))],
        compiler_params=pltpu.CompilerParams(has_side_effects=True, vmem_limit_bytes=VMEM_LIMIT),
    )(taken, x, wg, wu, wd)
    return outs[0]


CHUNKS = 16
LOADS = 4


def combine_kernel(first, second, gate0, gate1, results, out, held, wide, tile, done,
                   load_s, own_s, core_s, core_r, y_s, y_r, fwd_s, fwd_r):
    dp, z, tp = lax.axis_index('dp'), lax.axis_index('ep'), lax.axis_index('tp')
    y, c = tp // 2, tp % 2
    n_res, cols = results.shape
    chunk = done.shape[1]
    peer_core, peer_chip = 2 * y + 1 - c, 2 * (1 - y) + c

    def place(b, quarter):
        return out.at[pl.ds(pl.multiple_of(b * chunk, 16), chunk), pl.ds(pl.multiple_of(quarter * cols, 128), cols)]

    def remote(src, dst, send, recv, device):
        return pltpu.make_async_remote_copy(src_ref=src, dst_ref=dst, send_sem=send, recv_sem=recv,
                                            device_id=(dp, z, device), device_id_type=MESH)

    def own(b):
        return pltpu.make_async_copy(done.at[b], place(b, tp), own_s.at[b])

    def to_core(b):
        return remote(done.at[b], place(b, tp), core_s.at[b], core_r.at[b], peer_core)

    def to_chip(b):
        return remote(done.at[b], place(b, tp), y_s.at[b], y_r.at[b], peer_chip)

    def forward(b):
        return remote(place(b, peer_chip), place(b, peer_chip), fwd_s.at[b], fwd_r.at[b], peer_core)

    load_rows = n_res // LOADS
    block = load_rows // 4

    def load(i):
        at = pl.ds(i * load_rows, load_rows)
        return pltpu.make_async_copy(results.at[at], held.at[at], load_s.at[i])

    def widen(r, carry):
        at = pl.ds(pl.multiple_of(r * block, 8), block)
        wide[at, :] = held[at, :].astype(jnp.float32)
        return carry

    for i in range(LOADS):
        load(i).start()
    wide[pl.ds(n_res, 8), :] = jnp.zeros((8, cols), jnp.float32)
    for i in range(LOADS):
        load(i).wait()
        lax.fori_loop(4 * i, 4 * i + 4, widen, 0)
    part = tile.shape[0]

    def part_body(i, carry):
        def eight(g, carry):
            for u in range(8):
                t = i * part + g * 8 + u
                row = gate0[t] * wide[pl.ds(first[t], 1), :] + gate1[t] * wide[pl.ds(second[t], 1), :]
                tile[pl.ds(g * 8 + u, 1), :] = row
            return carry

        lax.fori_loop(0, part // 8, eight, 0)
        per = chunk // part
        b = i // per
        done[b, pl.ds(pl.multiple_of(i % per * part, 16), part), :] = tile[...].astype(jnp.bfloat16)

        @pl.when(i % per == per - 1)
        def _():
            to_chip(b).start()
            to_core(b).start()
            own(b).start()
        return carry

    lax.fori_loop(0, CHUNKS * chunk // part, part_body, 0)
    for b in range(CHUNKS):
        to_chip(b).wait_recv()
        forward(b).start()
    for b in range(CHUNKS):
        own(b).wait()
        to_chip(b).wait_send()
        to_core(b).wait_send()
        forward(b).wait_send()
        to_core(b).wait_recv()
        forward(b).wait_recv()


def run_combine(index, gates, results):
    tokens = index.shape[1]
    cols = results.shape[1]
    chunk = tokens // CHUNKS
    bf16, dma = jnp.bfloat16, pltpu.SemaphoreType.DMA
    smem = pl.BlockSpec(memory_space=pltpu.SMEM)
    return pl.pallas_call(
        combine_kernel,
        name='moe_combine',
        out_shape=jax.ShapeDtypeStruct((tokens, 4 * cols), bf16),
        in_specs=[smem] * 4 + [ANY],
        out_specs=ANY,
        scratch_shapes=[pltpu.VMEM(results.shape, bf16),
                        pltpu.VMEM((results.shape[0] + 8, cols), jnp.float32),
                        pltpu.VMEM((min(256, chunk), cols), jnp.float32),
                        pltpu.VMEM((CHUNKS, chunk, cols), bf16),
                        dma((LOADS,)), *[dma((CHUNKS,)) for _ in range(7)]],
        compiler_params=pltpu.CompilerParams(has_side_effects=True, vmem_limit_bytes=VMEM_LIMIT),
    )(index[0], index[1], gates[0], gates[1], results)


def solution(mesh):
    n_ep = mesh.shape['ep']
    row_spec = P(('dp', 'ep'), None)

    def device_body(x_loc, ids_loc, gates_loc, wg_loc, wu_loc, wd_loc):
        tokens, d_model = x_loc.shape
        n_top = ids_loc.shape[1]
        local_experts = wg_loc.shape[0]
        n_experts = local_experts * n_ep
        capacity = CAP_NUM * n_top * tokens // (CAP_DEN * n_experts)
        parity = lax.axis_index('tp') // 2
        chosen, slots = slot_numbers(ids_loc, n_experts)
        taken = jnp.where(chosen, slots, -1).reshape(n_ep, local_experts, tokens)
        taken = lax.dynamic_index_in_dim(taken, parity, axis=1, keepdims=False)
        ids_t = ids_loc.T
        expert = jnp.arange(n_experts, dtype=jnp.int32)[None, :, None]
        copy_slot = jnp.sum(jnp.where(ids_t[:, None, :] == expert, slots[None], 0), axis=1)
        index = jnp.where(copy_slot < capacity, ids_t * capacity + copy_slot, n_experts * capacity)
        results = run_layer(taken.reshape(n_ep, tokens // 128, 128), x_loc, capacity // 2, wg_loc, wu_loc, wd_loc)
        results = results.reshape(n_experts * capacity, d_model // 4)
        return run_combine(index, gates_loc.T, results)

    return jax.shard_map(device_body, mesh=mesh,
                         in_specs=(row_spec, row_spec, row_spec, P('ep', None, 'tp'), P('ep', None, 'tp'), P('ep', 'tp', None)),
                         out_specs=row_spec, check_vma=False)
```
